128 devices in a mesh: gx: 128 (over z, y, x, core).
Axes of the slice: x: 4, y: 4, z: 4, core: 2. Of those that a mesh axis runs over, the one named last changes fastest.
Arguments:
- value: float32 [256, 48, 32, 128], P('gx'), may hold values from -6 to 6
- target: float32 [256, 48, 32, 128], P('gx'), may hold values from -6 to 6
- obstacle: float32 [256, 48, 32, 128], P('gx'), may hold values from -6 to -0.5
- fractions: float32 [16, 4], replicated, may hold values from 0 to 1
- control_cost: float32 [16], replicated, may hold values from 0 to 0.5
- shard_offset: int32 [16], replicated, may hold values from -8 to 8, as said below
- cell_offset: int32 [16], replicated, may hold values from 0 to 1
- grid_offset: int32 [16, 3], replicated, may hold values from -4 to 4
Outputs:
- updated: float32 [256, 48, 32, 128], P('gx')
The draws below stay inside these ranges and needn't reach their ends.
Inputs may be any that keep to these rules, and one draw needn't show every extreme that they name: `shard_offset`: every draw holds both -8 and 8.
All inputs are finite; a program needn't handle non-finite values.
Results may differ from the reference program's by a relative error of at most 0.00002.
Values sent between devices are 32-bit elements; how exact they have to be, the bound alone decides.
No kernel may reach another device: no remote copies, remote signals or barrier semaphores. Data moves between devices by JAX's collectives and lax.ppermute only.
A program may use at most 128 MiB of HBM per device.

```python
import jax
import jax.numpy as jnp
from jax import lax

CX = 2
NY = 48
NZ = 32
NW = 128
NCTRL = 16
REACH = 8
NX = 256


def draw_shard_offset(key, part):
    first_key, second_key = jax.random.split(jax.random.fold_in(key, 11))
    offsets = jax.random.randint(first_key, (NCTRL,), -REACH, REACH + 1)
    order = jax.random.permutation(second_key, NCTRL)
    offsets = offsets.at[order[0]].set(-REACH).at[order[1]].set(REACH)
    return offsets.astype(jnp.int32)


def set_ends(entries, own_key, smallest, top_value):
    index_at = [jax.random.randint(jax.random.fold_in(own_key, axis), (), 0, length) for axis, length in enumerate(entries.shape)]
    widest = entries.shape.index(max(entries.shape))
    neighbour = index_at[:widest] + [(index_at[widest] + 1) % entries.shape[widest]] + index_at[widest + 1:]
    return entries.at[tuple(index_at)].set(smallest).at[tuple(neighbour)].set(top_value)


def block_levels(own_key, shape, cuts, low, high):
    def one(axis_at, blocks):
        heights = jax.random.uniform(jax.random.fold_in(jax.random.fold_in(own_key, 6), axis_at), (blocks,), jnp.float32, low / len(cuts), high / len(cuts))
        return jnp.repeat(jnp.exp(heights), shape[axis_at] // blocks).reshape((-1,) + (1,) * (len(shape) - axis_at - 1))

    level = one(*cuts[0])
    for cut in cuts[1:]:
        level = level * one(*cut)
    return level


def bell_draw(own_key, extent, width, reach, cuts=(), held_as=jnp.bfloat16):
    gain = block_levels(own_key, extent, cuts, -0.22, 0.18) if cuts else 1.0
    array = jax.random.normal(own_key, extent, jnp.float32) * width * gain
    return jnp.minimum(jnp.maximum(array, -reach), reach).astype(held_as)


def setup_inputs(seed: int = 0) -> dict:
    arg_keys = jax.random.split(jax.random.key(seed), 9)
    value = bell_draw(arg_keys[0], (NX, NY, NZ, NW), 1.0, 6.0, ((0, 128),), jnp.float32)
    target = bell_draw(arg_keys[1], (NX, NY, NZ, NW), 1.0, 6.0, ((0, 128),), jnp.float32)
    obstacle = jnp.clip(-6.0 + 5.5 * jax.random.uniform(arg_keys[2], (NX, NY, NZ, NW), jnp.float32) ** block_levels(arg_keys[2], (NX, NY, NZ, NW), ((0, 128),), -0.2, 0.2), -6.0, -0.5)
    fractions = jnp.clip(jax.random.uniform(arg_keys[3], (NCTRL, 4), jnp.float32, 0.0, 1.0), 0.0, 1.0)
    control_cost = jnp.clip(jax.random.uniform(arg_keys[4], (NCTRL,), jnp.float32, 0.0, 0.5), 0.0, 0.5)
    shard_offset = draw_shard_offset(jax.random.fold_in(arg_keys[8], 71), 0)
    cell_offset = set_ends(jax.random.randint(arg_keys[6], (NCTRL,), 0, CX), jax.random.fold_in(arg_keys[6], 1), 0, CX - 1).astype(jnp.int32)
    grid_offset = set_ends(jax.random.randint(arg_keys[7], (NCTRL, 3), -4, 5), jax.random.fold_in(arg_keys[7], 1), -4, 4).astype(jnp.int32)
    return {"value": value, "target": target, "obstacle": obstacle, "fractions": fractions, "control_cost": control_cost, "shard_offset": shard_offset, "cell_offset": cell_offset, "grid_offset": grid_offset}


def blend(low, high, frac):
    return (1.0 - frac) * low + frac * high


def reference(value, target, obstacle, fractions, control_cost, shard_offset, cell_offset, grid_offset):
    def one_control(u, best):
        along = (shard_offset[u] * CX + cell_offset[u]).astype(jnp.int32)
        field = blend(jnp.roll(value, -along, axis=0), jnp.roll(value, -along - 1, axis=0), fractions[u, 0])
        for axis_k in range(1, 4):
            moved = grid_offset[u, axis_k - 1].astype(jnp.int32)
            field = blend(jnp.roll(field, -moved, axis=axis_k), jnp.roll(field, -moved - 1, axis=axis_k), fractions[u, axis_k])
        return jnp.minimum(best, field + control_cost[u])

    start = jnp.full(value.shape, jnp.inf, jnp.float32)
    best = lax.fori_loop(0, NCTRL, one_control, start)
    return jnp.maximum(obstacle, jnp.minimum(target, best))
```

```python
import functools

import jax
import jax.numpy as jnp
import numpy as np
from jax import lax
from jax.experimental import pallas as pl
from jax.experimental.pallas import tpu as pltpu
from jax.sharding import PartitionSpec as P

NCTRL = 16
ROW = 8
NX4 = 4
UNROLL = 16

HBM = pltpu.MemorySpace.HBM
SMEM = pltpu.MemorySpace.SMEM

OWN, SIB, PA, PB, XA, XB, Q, XQ, HA, HXA, HB, HXB = range(12)
N_EARLY = 6


def source_table():
    table = np.zeros((ROW, 9), np.int32)
    for i in range(ROW):
        x, c = i // 2, i % 2
        first = -1 if x % 2 == 0 else 0
        for q in range(9):
            s = first + q
            if s < 0 or s >= ROW:
                if x in (1, 2):
                    direct = 0 if x == 1 else 1
                    table[i, q] = HA if c == direct else HXA
                else:
                    direct = 0 if x == 3 else 1
                    table[i, q] = HB if c == direct else HXB
                continue
            other = (s % 2) != c
            delta = (s // 2 - x) % NX4
            if delta == 0:
                table[i, q] = SIB if other else OWN
            elif delta == 2:
                table[i, q] = XQ if other else Q
            elif (delta == 1) == (c == 0):
                table[i, q] = XA if other else PB
                if delta == 3:
                    table[i, q] = XA if other else PB
            else:
                table[i, q] = XB if other else PA
    return table


def pairs(count, rule):
    out = []
    for d in range(count):
        r, i = divmod(d, ROW)
        to = rule(r, i // 2, i % 2)
        if to is None:
            continue
        r2, x2, c2 = to
        out.append((d, (r2 % (count // ROW)) * ROW + (x2 % NX4) * 2 + c2))
    return out


def blend(low, high, keep, frac):
    return keep * low + frac * high


def control_kernel(mode, nsrc, *refs):
    meta, so, co, goff, frac, cost = refs[:6]
    src = refs[6:6 + nsrc]
    refs = refs[6 + nsrc:]
    nbest = 1 if mode == "rest" else 2
    ninit = {"early": 0, "late": 2, "rest": 1}[mode]
    init, refs = refs[:ninit], refs[ninit:]
    outs, refs = refs[:nbest], refs[nbest:]
    buf, best, todo, sem, io_sem = refs
    ny, nz = best.shape[2], best.shape[3]

    inits = [pltpu.make_async_copy(init[b], best.at[b], io_sem.at[b]) for b in range(ninit)]
    for copy in inits:
        copy.start()

    i, first = meta[0], meta[1]

    def place(u):
        at = i + so[u] - first
        a = jnp.where(at < 0, -1, jnp.where(at >= ROW, 1, 0))
        return a, at - a * ROW

    def listed(u, n):
        a, q = place(u)
        early = jnp.logical_and(meta[2 + q] < N_EARLY, meta[3 + q] < N_EARLY)
        if mode == "rest":
            take = a == 0
        elif mode == "early":
            take = jnp.logical_and(a != 0, early)
        else:
            take = jnp.logical_and(a != 0, jnp.logical_not(early))

        @pl.when(take)
        def _():
            todo[n] = u

        return n + take.astype(jnp.int32)

    count = lax.fori_loop(0, NCTRL, listed, jnp.int32(0))

    def row_copies(ref, half, slot, t):
        return (
            pltpu.make_async_copy(ref.at[half], buf.at[slot, t, :, pl.ds(0, nz), :], sem.at[slot]),
            pltpu.make_async_copy(
                ref.at[half, :, pl.ds(0, 8), :], buf.at[slot, t, :, pl.ds(nz, 8), :], sem.at[slot]
            ),
        )

    def fetch(k):
        u = todo[k]
        slot = lax.rem(k, 2)
        _, q = place(u)

        @pl.loop(0, 3)
        def _(t):
            at = co[u] + t
            half = jnp.bitwise_and(at, 1)
            which = meta[2 + q + jnp.right_shift(at, 1)]
            for n in range(nsrc):

                @pl.when(which == n)
                def _(n=n):
                    for copy in row_copies(src[n], half, slot, t):
                        copy.start()

    def compute(k):
        u = todo[k]
        slot = lax.rem(k, 2)
        a, _ = place(u)
        b = 0 if mode == "rest" else jnp.where(a > 0, 0, 1)
        f = [frac[4 * u + d] for d in range(4)]
        g = [1.0 - x for x in f]
        g1, g2, g3 = (goff[3 * u + d] for d in range(3))
        pay = cost[u]
        low, high = [], []
        for v in range(nz // 8):
            s = 8 * v + g2
            low.append(jnp.where(s < 0, s + nz, s))
            high.append(jnp.where(s + 1 < 0, s + 1 + nz, s + 1))
        turn0 = lax.rem(128 - g3, 128)
        turn1 = lax.rem(127 - g3, 128)

        def plane(y):
            y = jnp.where(y < 0, y + ny, y)
            y = jnp.where(y >= ny, y - ny, y)
            out = [[], []]
            for v in range(nz // 8):
                z = [
                    blend(buf[slot, t, y, pl.ds(low[v], 8), :], buf[slot, t, y, pl.ds(high[v], 8), :], g[2], f[2])
                    for t in range(3)
                ]
                out[0].append(blend(z[0], z[1], g[0], f[0]))
                out[1].append(blend(z[1], z[2], g[0], f[0]))
            return out[0] + out[1]

        def step(m, here):
            for n in range(UNROLL):
                y = m * UNROLL + n
                there = plane(y + g1 + 1)
                for row in range(2):
                    for v in range(nz // 8):
                        w = row * (nz // 8) + v
                        mid = blend(here[w], there[w], g[1], f[1])
                        full = blend(pltpu.roll(mid, turn0, 1), pltpu.roll(mid, turn1, 1), g[3], f[3])
                        at = (b, row, y, pl.ds(8 * v, 8), slice(None))
                        best[at] = jnp.minimum(best[at], full + pay)
                here = there
            return here

        lax.fori_loop(0, ny // UNROLL, step, plane(g1))

    @pl.when(count > 0)
    def _():
        fetch(jnp.int32(0))

    if not ninit:

        @pl.loop(0, ny)
        def _(y):
            for b in range(nbest):
                for row in range(2):
                    best[b, row, y] = jnp.full(best.shape[3:], jnp.inf, jnp.float32)

    for copy in inits:
        copy.wait()

    @pl.loop(0, count)
    def _(k):
        @pl.when(k + 1 < count)
        def _():
            fetch(k + 1)

        @pl.loop(0, 3)
        def _(t):
            for copy in row_copies(src[0], 0, lax.rem(k, 2), t):
                copy.wait()

        compute(k)

    ends = [pltpu.make_async_copy(best.at[b], outs[b], io_sem.at[b]) for b in range(nbest)]
    for copy in ends:
        copy.start()
    for copy in ends:
        copy.wait()


def run_controls(mode, params, sources, init, flops):
    shape = sources[0].shape
    nbest = 1 if mode == "rest" else 2
    out = jax.ShapeDtypeStruct(shape, jnp.float32)
    return pl.pallas_call(
        functools.partial(control_kernel, mode, len(sources)),
        out_shape=[out] * nbest,
        in_specs=[pl.BlockSpec(memory_space=SMEM)] * len(params)
        + [pl.BlockSpec(memory_space=HBM)] * (len(sources) + len(init)),
        out_specs=[pl.BlockSpec(memory_space=HBM)] * nbest,
        scratch_shapes=[
            pltpu.VMEM((2, 3, shape[1], shape[2] + 8, shape[3]), jnp.float32),
            pltpu.VMEM((nbest,) + shape, jnp.float32),
            pltpu.SMEM((NCTRL,), jnp.int32),
            pltpu.SemaphoreType.DMA((2,)),
            pltpu.SemaphoreType.DMA((2,)),
        ],
        compiler_params=pltpu.CompilerParams(vmem_limit_bytes=24 * 2**20),
        cost_estimate=pl.CostEstimate(flops=flops, bytes_accessed=2**20, transcendentals=0),
        name="controls_" + mode,
    )(*params, *sources, *init)


def body(value, target, obstacle, fractions, control_cost, shard_offset, cell_offset, grid_offset):
    size = lax.axis_size("gx")

    def move(x, rule):
        return lax.ppermute(x, "gx", pairs(size, rule))

    swap = lambda r, x, c: (r, x, 1 - c)
    chips = lambda members, rule: lambda r, x, c: rule(r, x, c) if x in members else None

    pa = move(value, lambda r, x, c: (r, x + 1 - 2 * c, c))
    pb = move(value, lambda r, x, c: (r, x - 1 + 2 * c, c))
    sib = move(value, swap)
    q = move(pa, lambda r, x, c: (r, x + 1 - 2 * c, c))
    xa = move(pa, swap)
    xb = move(pb, swap)
    halo = lambda up, down: lambda r, x, c: (
        (r - 1, x, c) if (x, c) == up else (r + 1, x, c) if (x, c) == down else None
    )
    ha = move(pa, halo((1, 0), (2, 1)))
    hb = move(pb, halo((3, 0), (0, 1)))
    hxa = move(ha, lambda r, x, c: (r, x, 1 - c) if (x, c) in ((1, 0), (2, 1)) else None)
    hxb = move(hb, lambda r, x, c: (r, x, 1 - c) if (x, c) in ((3, 0), (0, 1)) else None)
    xq = move(q, swap)

    i = lax.rem(lax.axis_index("gx"), ROW)
    table = source_table()
    first = np.array([-1 if (k // 2) % 2 == 0 else 0 for k in range(ROW)], np.int32)
    meta = jnp.asarray(np.concatenate([np.arange(ROW, dtype=np.int32)[:, None], first[:, None], table], 1))
    meta = lax.dynamic_index_in_dim(meta, i, 0, keepdims=False)
    params = (
        meta,
        shard_offset,
        cell_offset,
        grid_offset.reshape(-1),
        fractions.reshape(-1),
        control_cost,
    )
    early = [value, sib, pa, pb, xa, xb]
    full = early + [q, xq, ha, hxa, hb, hxb]
    up, down = run_controls("early", params, early, [], 2 * 10**7)
    up, down = run_controls("late", params, full, [up, down], 10**7)
    got_up = move(up, lambda r, x, c: (r - 1, x, c))
    got_down = move(down, lambda r, x, c: (r + 1, x, c))
    (mine,) = run_controls("rest", params, full, [target], 3 * 10**7)
    return jnp.maximum(obstacle, jnp.minimum(mine, jnp.minimum(got_up, got_down)))


def solution(mesh):
    return jax.shard_map(
        body,
        mesh=mesh,
        in_specs=(
            P("gx", None, None, None),
            P("gx", None, None, None),
            P("gx", None, None, None),
            P(),
            P(),
            P(),
            P(),
            P(),
        ),
        out_specs=P("gx", None, None, None),
        check_vma=False,
    )
```

```python
import functools

import jax
import jax.numpy as jnp
from jax import lax
from jax.experimental import pallas as pl
from jax.experimental.pallas import tpu as pltpu
from jax.sharding import PartitionSpec as P


NCTRL = 16
ROW = 8
NX4 = 4
UNROLL = 16
VMEM_LIMIT = 60 * 2**20

HBM = pltpu.MemorySpace.HBM
SMEM = pltpu.MemorySpace.SMEM

OWN, SIB, PA, PB, XA, XB, Q, XQ, HA, HXA, HB, HXB = range(12)
N_EARLY = 6


def source_of(i, s):
    x, c = jnp.right_shift(i, 1), jnp.bitwise_and(i, 1)
    other = jnp.bitwise_and(s, 1) != c
    delta = jnp.bitwise_and(jnp.right_shift(s, 1) - x, NX4 - 1)
    near = jnp.where(
        (delta == 1) == (c == 0), jnp.where(other, XA, PB), jnp.where(other, XB, PA)
    )
    inside = jnp.where(
        delta == 0,
        jnp.where(other, SIB, OWN),
        jnp.where(delta == 2, jnp.where(other, XQ, Q), near),
    )
    middle = jnp.logical_or(x == 1, x == 2)
    direct = jnp.where(jnp.bitwise_and(x, 1) == 1, 0, 1) == c
    halo = jnp.where(middle, jnp.where(direct, HA, HXA), jnp.where(direct, HB, HXB))
    return jnp.where(jnp.logical_or(s < 0, s >= ROW), halo, inside)


def pairs(count, rule):
    out = []
    for d in range(count):
        r, i = divmod(d, ROW)
        to = rule(r, i // 2, i % 2)
        if to is None:
            continue
        r2, x2, c2 = to
        out.append((d, (r2 % (count // ROW)) * ROW + (x2 % NX4) * 2 + c2))
    return out


def blend(low, high, keep, frac):
    return keep * low + frac * high


def control_kernel(mode, nsrc, *refs):
    so, co, goff, frac, cost = refs[:5]
    src = refs[5:5 + nsrc]
    refs = refs[5 + nsrc:]
    nbest = 1 if mode == "rest" else 2
    ninit = {"early": 0, "late": 2, "rest": 1}[mode]
    init, refs = refs[:ninit], refs[ninit:]
    outs, refs = refs[:nbest], refs[nbest:]
    buf, best, todo, where, sem, io_sem = refs
    ny, nz = best.shape[2], best.shape[3]

    inits = [pltpu.make_async_copy(init[b], best.at[b], io_sem.at[b]) for b in range(ninit)]
    for copy in inits:
        copy.start()

    i = lax.rem(lax.axis_index("gx"), ROW)
    first = -jnp.bitwise_and(1 - jnp.right_shift(i, 1), 1)
    for q in range(9):
        where[q] = source_of(i, first + q)

    def place(u):
        at = i + so[u] - first
        a = jnp.where(at < 0, -1, jnp.where(at >= ROW, 1, 0))
        return a, at - a * ROW

    def listed(u, n):
        a, q = place(u)
        early = jnp.logical_and(where[q] < N_EARLY, where[q + 1] < N_EARLY)
        if mode == "rest":
            take = a == 0
        elif mode == "early":
            take = jnp.logical_and(a != 0, early)
        else:
            take = jnp.logical_and(a != 0, jnp.logical_not(early))

        @pl.when(take)
        def _():
            todo[n] = u

        return n + take.astype(jnp.int32)

    count = lax.fori_loop(0, NCTRL, listed, jnp.int32(0))

    def row_copies(ref, half, slot, t):
        return (
            pltpu.make_async_copy(ref.at[half], buf.at[slot, t, :, pl.ds(0, nz), :], sem.at[slot]),
            pltpu.make_async_copy(
                ref.at[half, :, pl.ds(0, 8), :], buf.at[slot, t, :, pl.ds(nz, 8), :], sem.at[slot]
            ),
        )

    def fetch(k):
        u = todo[k]
        slot = lax.rem(k, 2)
        _, q = place(u)

        @pl.loop(0, 3)
        def _(t):
            at = co[u] + t
            half = jnp.bitwise_and(at, 1)
            which = where[q + jnp.right_shift(at, 1)]
            for n in range(nsrc):

                @pl.when(which == n)
                def _(n=n):
                    for copy in row_copies(src[n], half, slot, t):
                        copy.start()

    def compute(k):
        u = todo[k]
        slot = lax.rem(k, 2)
        a, _ = place(u)
        b = 0 if mode == "rest" else jnp.where(a > 0, 0, 1)
        f = [frac[u, d] for d in range(4)]
        g = [1.0 - x for x in f]
        g1, g2, g3 = (goff[u, d] for d in range(3))
        pay = cost[u]
        low, high = [], []
        for v in range(nz // 8):
            s = 8 * v + g2
            low.append(jnp.where(s < 0, s + nz, s))
            high.append(jnp.where(s + 1 < 0, s + 1 + nz, s + 1))
        turn0 = lax.rem(128 - g3, 128)
        turn1 = lax.rem(127 - g3, 128)

        def plane(y):
            y = jnp.where(y < 0, y + ny, y)
            y = jnp.where(y >= ny, y - ny, y)
            out = [[], []]
            for v in range(nz // 8):
                z = [
                    blend(buf[slot, t, y, pl.ds(low[v], 8), :], buf[slot, t, y, pl.ds(high[v], 8), :], g[2], f[2])
                    for t in range(3)
                ]
                out[0].append(blend(z[0], z[1], g[0], f[0]))
                out[1].append(blend(z[1], z[2], g[0], f[0]))
            return out[0] + out[1]

        def step(m, here):
            for n in range(UNROLL):
                y = m * UNROLL + n
                there = plane(y + g1 + 1)
                for row in range(2):
                    for v in range(nz // 8):
                        w = row * (nz // 8) + v
                        mid = blend(here[w], there[w], g[1], f[1])
                        full = blend(pltpu.roll(mid, turn0, 1), pltpu.roll(mid, turn1, 1), g[3], f[3])
                        at = (b, row, y, pl.ds(8 * v, 8), slice(None))
                        best[at] = jnp.minimum(best[at], full + pay)
                here = there
            return here

        lax.fori_loop(0, ny // UNROLL, step, plane(g1))

    @pl.when(count > 0)
    def _():
        fetch(jnp.int32(0))

    if not ninit:

        @pl.loop(0, ny)
        def _(y):
            for b in range(nbest):
                for row in range(2):
                    best[b, row, y] = jnp.full(best.shape[3:], jnp.inf, jnp.float32)

    for copy in inits:
        copy.wait()

    @pl.loop(0, count)
    def _(k):
        @pl.when(k + 1 < count)
        def _():
            fetch(k + 1)

        @pl.loop(0, 3)
        def _(t):
            for copy in row_copies(src[0], 0, lax.rem(k, 2), t):
                copy.wait()

        compute(k)

    ends = [pltpu.make_async_copy(best.at[b], outs[b], io_sem.at[b]) for b in range(nbest)]
    for copy in ends:
        copy.start()
    for copy in ends:
        copy.wait()


def run_controls(mode, params, sources, init, flops):
    shape = sources[0].shape
    nbest = 1 if mode == "rest" else 2
    out = jax.ShapeDtypeStruct(shape, jnp.float32)
    return pl.pallas_call(
        functools.partial(control_kernel, mode, len(sources)),
        out_shape=[out] * nbest,
        in_specs=[pl.BlockSpec(memory_space=SMEM)] * len(params)
        + [pl.BlockSpec(memory_space=HBM)] * (len(sources) + len(init)),
        out_specs=[pl.BlockSpec(memory_space=HBM)] * nbest,
        scratch_shapes=[
            pltpu.VMEM((2, 3, shape[1], shape[2] + 8, shape[3]), jnp.float32),
            pltpu.VMEM((nbest,) + shape, jnp.float32),
            pltpu.SMEM((NCTRL,), jnp.int32),
            pltpu.SMEM((9,), jnp.int32),
            pltpu.SemaphoreType.DMA((2,)),
            pltpu.SemaphoreType.DMA((2,)),
        ],
        compiler_params=pltpu.CompilerParams(vmem_limit_bytes=VMEM_LIMIT),
        cost_estimate=pl.CostEstimate(flops=flops, bytes_accessed=2**20, transcendentals=0),
    )(*params, *sources, *init)


def body(value, target, obstacle, fractions, control_cost, shard_offset, cell_offset, grid_offset):
    size = lax.axis_size("gx")

    def move(x, rule):
        return lax.ppermute(x, "gx", pairs(size, rule))

    swap = lambda r, x, c: (r, x, 1 - c)
    forth = lambda r, x, c: (r, x + 1 - 2 * c, c)
    back = lambda r, x, c: (r, x - 1 + 2 * c, c)
    halo = lambda up, down: lambda r, x, c: (
        (r - 1, x, c) if (x, c) == up else (r + 1, x, c) if (x, c) == down else None
    )
    swap_on = lambda *who: lambda r, x, c: (r, x, 1 - c) if (x, c) in who else None

    pa = move(value, forth)
    pb = move(value, back)
    sib = move(value, swap)
    q = move(pa, forth)
    xa = move(pa, swap)
    xb = move(pb, swap)
    ha = move(pa, halo((1, 0), (2, 1)))
    hb = move(pb, halo((3, 0), (0, 1)))
    xq = move(q, swap)
    hxa = move(ha, swap_on((1, 0), (2, 1)))
    hxb = move(hb, swap_on((3, 0), (0, 1)))

    params = (shard_offset, cell_offset, grid_offset, fractions, control_cost)
    near = [value, sib, pa, pb, xa, xb]
    full = near + [q, xq, ha, hxa, hb, hxb]
    up, down = run_controls("early", params, near, [], 2 * 10**7)
    up, down = run_controls("late", params, full, [up, down], 10**7)
    got_up = move(up, lambda r, x, c: (r - 1, x, c))
    got_down = move(down, lambda r, x, c: (r + 1, x, c))
    (mine,) = run_controls("rest", params, full, [target], 3 * 10**7)
    return jnp.maximum(obstacle, jnp.minimum(mine, jnp.minimum(got_up, got_down)))


def solution(mesh):
    return jax.shard_map(
        body,
        mesh=mesh,
        in_specs=(
            P("gx", None, None, None),
            P("gx", None, None, None),
            P("gx", None, None, None),
            P(),
            P(),
            P(),
            P(),
            P(),
        ),
        out_specs=P("gx", None, None, None),
        check_vma=False,
    )
```
